32 devices in a mesh: seq: 8 (over z, y), head: 4 (over x, core).
Axes of the slice: x: 2, y: 2, z: 4, core: 2. Of those that a mesh axis runs over, the one named last changes fastest.
Arguments:
- queries: bfloat16 [6144, 4096], P(('seq', 'head')), may hold values from -6 to 6
- key_rows: bfloat16 [6144, 4096], P(('seq', 'head')), may hold values from -6 to 6
- values: bfloat16 [6144, 4096], P(('seq', 'head')), may hold values from -6 to 6
- doc_ids: int32 [6144], replicated, may hold values from 0 to 15, as said below
- image_flags: int32 [6144], replicated, may hold values from 0 to 1, as said below
- labels: int32 [6144], P(('seq', 'head')), may hold values from -1 to 31999, as said below
- token_loss: float32 [6144], P(('seq', 'head')), may hold values from 0.05 to 8
Outputs:
- attended: bfloat16 [6144, 4096], P(('seq', 'head'))
- doc_count: float32 [16], replicated
- doc_loss: float32 [16], replicated
The draws below stay inside these ranges and needn't reach their ends.
Inputs may be any that keep to these rules, and one draw needn't show every extreme that they name: `doc_ids`: document numbers never fall along the sequence and rise by one from one document to the next; every document holds at least 64 and at most 704 tokens, and some document holds exactly 704. `image_flags`: the 1s form spans of exactly 576 consecutive tokens, at most one span a document, each inside one document and never at its first token. `labels`: every image token has -1, and some document has -1 on all of its tokens.
All inputs are finite; a program needn't handle non-finite values.
Results may differ from the reference program's by a relative error of at most 0.0034.
Values may be sent and summed in bfloat16 or wider, within the bound.
No kernel may reach another device: no remote copies, remote signals or barrier semaphores. Data moves between devices by JAX's collectives and lax.ppermute only.
A program may use at most 128 MiB of HBM per device.

```python
import math
import jax
import jax.numpy as jnp
from jax import lax

HEADS = 32
HEAD_DIM = 128
VOCAB = 32000
TOK_DEV = 768
DOC_MEAN = 384
DOC_MOST = 704
IMG_LEN = 576
TOKENS = 6144
DOCS = 16
N_SEQ = 8


def layout(key):
    base = jax.random.fold_in(key, 7001)
    spare = (DOC_MOST - DOC_MEAN) // 2
    ratio = TOK_DEV // DOC_MEAN
    offsets = jax.random.randint(jax.random.fold_in(base, 1), (DOCS + 1,), -spare, spare + 1).astype(jnp.int32)
    offsets = offsets.at[0].set(0).at[DOCS].set(0)
    lowest = max(1, IMG_LEN + 1 - DOC_MEAN - spare)
    reach = jax.random.randint(jax.random.fold_in(base, 2), (N_SEQ - 1,), lowest, spare + 1).astype(jnp.int32)
    picked = jax.random.randint(jax.random.fold_in(base, 3), (), 0, N_SEQ - 1)
    reach = reach.at[picked].set(spare)
    block_index = jnp.arange(1, N_SEQ, dtype=jnp.int32)
    boundary_doc = block_index * ratio
    offsets = offsets.at[boundary_doc - 1].set(-spare)
    offsets = offsets.at[boundary_doc].set(reach)
    bounds = (jnp.arange(DOCS + 1, dtype=jnp.int32) * DOC_MEAN + offsets).astype(jnp.int32)
    starts = bounds[:-1]
    ends = bounds[1:]
    lengths = ends - starts
    places = jnp.arange(TOKENS, dtype=jnp.int32)
    docs = jnp.searchsorted(ends, places, side='right').astype(jnp.int32)
    room = lengths - IMG_LEN
    offset = 1 + jax.random.randint(jax.random.fold_in(base, 4), (DOCS,), 0, jnp.maximum(room, 1))
    chosen = (jax.random.randint(jax.random.fold_in(base, 5), (DOCS,), 0, 2) == 1) & (room >= 1)
    image_start = (starts + offset).astype(jnp.int32)
    image_start = image_start.at[boundary_doc - 1].set(block_index * TOK_DEV + reach - IMG_LEN)
    chosen = chosen.at[boundary_doc - 1].set(True)
    flags = chosen[docs] & (places >= image_start[docs]) & (places < image_start[docs] + IMG_LEN)
    return (docs, flags.astype(jnp.int32))


def draw_doc_ids(key, part):
    return layout(key)[0]


def draw_image_flags(key, part):
    return layout(key)[1]


def draw_labels(key, part):
    docs, flags = layout(key)
    token_ids = jax.random.randint(jax.random.fold_in(key, 7101), (TOKENS,), 0, VOCAB)
    dropped = jax.random.randint(jax.random.fold_in(key, 7102), (TOKENS,), 0, 8) == 0
    silent = jax.random.randint(jax.random.fold_in(key, 7103), (2,), 0, DOCS)
    muted = (docs == silent[0]) | (docs == silent[1])
    return jnp.where((flags == 1) | dropped | muted, -1, token_ids).astype(jnp.int32)


def draw_queries(key, part):
    columns = HEADS * HEAD_DIM
    field = jnp.clip(jax.random.normal(jax.random.fold_in(key, 7303), (TOKENS, columns), jnp.float32), -5.0, 5.0)
    return field.astype(jnp.bfloat16)


def draw_key_rows(key, part):
    columns = HEADS * HEAD_DIM
    field = jnp.clip(jax.random.normal(jax.random.fold_in(key, 7403), (TOKENS, columns), jnp.float32), -5.0, 5.0)
    return field.astype(jnp.bfloat16)


def block_scale(own_key, dims, split, least, high):
    def one(dim, parts):
        heights = jax.random.uniform(jax.random.fold_in(jax.random.fold_in(own_key, 6), dim), (parts,), jnp.float32, least / len(split), high / len(split))
        return jnp.repeat(jnp.exp(heights), dims[dim] // parts).reshape((-1,) + (1,) * (len(dims) - dim - 1))

    level = one(*split[0])
    for cut in split[1:]:
        level = level * one(*cut)
    return level


def noise(key, extent, deviation, most, split=(), kind=jnp.bfloat16):
    result = deviation * jax.random.normal(key, extent, jnp.float32)
    if split:
        result = result * block_scale(key, extent, split, -0.22, 0.18)
    return jnp.clip(result, -most, most).astype(kind)


def setup_inputs(seed: int = 0) -> dict:
    arg_keys = jax.random.split(jax.random.key(seed), 8)
    return {
        "queries": draw_queries(jax.random.fold_in(arg_keys[7], 71), 0),
        "key_rows": draw_key_rows(jax.random.fold_in(arg_keys[7], 71), 0),
        "values": noise(arg_keys[2], (TOKENS, HEADS * HEAD_DIM), 1.0, 6.0, ((0, 32),)),
        "doc_ids": draw_doc_ids(jax.random.fold_in(arg_keys[7], 71), 0),
        "image_flags": draw_image_flags(jax.random.fold_in(arg_keys[7], 71), 0),
        "labels": draw_labels(jax.random.fold_in(arg_keys[7], 71), 0),
        "token_loss": jnp.clip(jnp.exp(math.log(8.0) - 5.075174 * jax.random.uniform(arg_keys[6], (TOKENS,), jnp.float32) ** block_scale(arg_keys[6], (TOKENS,), ((0, 32),), -0.2, 0.2)), 0.05, 8.0),
    }


def allowed_pairs(query_docs, query_flags, query_places, key_docs, key_flags, key_places):
    same = query_docs[:, None] == key_docs[None, :]
    earlier = key_places[None, :] <= query_places[:, None]
    image = (query_flags[:, None] == 1) & (key_flags[None, :] == 1)
    return same & (earlier | image)


def attend(query_part, key_window, value_window, allowed):
    outputs = []
    scale = HEAD_DIM ** -0.5
    for head_index in range(query_part.shape[1] // HEAD_DIM):
        lower = head_index * HEAD_DIM
        query_head = query_part[:, lower:lower + HEAD_DIM]
        key_head = key_window[:, lower:lower + HEAD_DIM]
        value_head = value_window[:, lower:lower + HEAD_DIM]
        scores = lax.dot_general(query_head, key_head, (((1,), (1,)), ((), ())), preferred_element_type=jnp.float32) * scale
        scores = jnp.where(allowed, scores, -jnp.inf)
        row_max = jnp.max(scores, axis=1, keepdims=True)
        weights = jnp.exp(scores - row_max)
        total = jnp.sum(weights, axis=1, keepdims=True)
        mixed = jnp.dot(weights.astype(jnp.bfloat16), value_head, preferred_element_type=jnp.float32) / total
        outputs.append(mixed.astype(jnp.bfloat16))
    return jnp.concatenate(outputs, axis=1)


def reference(queries, key_rows, values, doc_ids, image_flags, labels, token_loss):
    reach_back = (DOC_MOST + TOK_DEV - 2) // TOK_DEV
    reach_front = (IMG_LEN + TOK_DEV - 2) // TOK_DEV
    window = (reach_back + 1 + reach_front) * TOK_DEV

    def one_block(index):
        query_start = index * TOK_DEV
        key_start = jnp.clip(query_start - reach_back * TOK_DEV, 0, TOKENS - window).astype(jnp.int32)
        query_part = lax.dynamic_slice_in_dim(queries, query_start, TOK_DEV, 0)
        key_window = lax.dynamic_slice_in_dim(key_rows, key_start, window, 0)
        value_window = lax.dynamic_slice_in_dim(values, key_start, window, 0)
        query_docs = lax.dynamic_slice_in_dim(doc_ids, query_start, TOK_DEV, 0)
        query_flags = lax.dynamic_slice_in_dim(image_flags, query_start, TOK_DEV, 0)
        key_docs = lax.dynamic_slice_in_dim(doc_ids, key_start, window, 0)
        key_flags = lax.dynamic_slice_in_dim(image_flags, key_start, window, 0)
        query_places = query_start + jnp.arange(TOK_DEV, dtype=jnp.int32)
        key_places = key_start + jnp.arange(window, dtype=jnp.int32)
        allowed = allowed_pairs(query_docs, query_flags, query_places, key_docs, key_flags, key_places)
        return attend(query_part, key_window, value_window, allowed)

    blocks = lax.map(one_block, jnp.arange(N_SEQ, dtype=jnp.int32))
    attended = blocks.reshape(TOKENS, queries.shape[1])
    documents = TOKENS // DOC_MEAN
    member = (doc_ids[:, None] == jnp.arange(documents, dtype=jnp.int32)[None, :]) & (labels[:, None] >= 0)
    doc_count = jnp.sum(member.astype(jnp.float32), axis=0)
    loss_sum = jnp.sum(jnp.where(member, token_loss[:, None], jnp.float32(0.0)), axis=0)
    doc_loss = loss_sum / jnp.maximum(doc_count, jnp.float32(1.0))
    return attended, doc_count, doc_loss
```

```python
import functools
import math

import jax
import jax.numpy as jnp
from jax import lax
from jax.experimental import pallas as pl
from jax.experimental.pallas import tpu as pltpu
from jax.sharding import Mesh, PartitionSpec as P

HEAD_DIM = 128
DOC_MEAN = 384
DOC_MOST = 704
IMG_LEN = 576
LEAST = -1e30
GRAIN = 64


def round_up(count, grain):
    return -(-count // grain) * grain


def shifted(block, axis, distance):
    devices = range(lax.axis_size(axis))
    route = [(i - distance, i) for i in devices if i - distance in devices]
    return lax.ppermute(block, axis, route)


def summed(totals, axis):
    size = lax.axis_size(axis)
    if size & (size - 1):
        return lax.psum(totals, axis)
    distance = 1
    while distance < size:
        totals = totals + lax.ppermute(totals, axis, [(i, i ^ distance) for i in range(size)])
        distance *= 2
    return totals


def attend_kernel(
    first_ref, count_ref, low_ref, span_ref, q_ref,
    k_back_ref, k_own_ref, k_ahead_ref, v_back_ref, v_own_ref, v_ahead_ref,
    out_ref, keys, mixed, scores, top, gathered, *, heads, width,
):
    step = pl.program_id(0)
    rows = q_ref.shape[0]
    window = keys.shape[0]
    back = k_back_ref.shape[0]
    own = k_own_ref.shape[0]
    ahead = k_ahead_ref.shape[0]
    factor = HEAD_DIM ** (-0.5) * math.log2(math.e)

    @pl.when(step == 0)
    def _():
        pieces = ((0, back, k_back_ref, v_back_ref), (back, own, k_own_ref, v_own_ref),
                  (back + own, ahead, k_ahead_ref, v_ahead_ref))
        ones = jnp.ones((window, HEAD_DIM), mixed.dtype)
        for start, length, key_part, value_part in pieces:
            keys[start:start + length, :] = key_part[...]
            for head in range(heads):
                lower = head * HEAD_DIM
                mixed[start:start + length, 2 * lower:2 * lower + HEAD_DIM] = (
                    value_part[:, lower:lower + HEAD_DIM])
        rest = window - back - own - ahead
        keys[window - rest:, :] = jnp.zeros((rest, keys.shape[1]), keys.dtype)
        for head in range(heads):
            lower = head * HEAD_DIM
            mixed[window - rest:, 2 * lower:2 * lower + HEAD_DIM] = jnp.zeros((rest, HEAD_DIM), mixed.dtype)
            mixed[:, 2 * lower + HEAD_DIM:2 * lower + 2 * HEAD_DIM] = ones

    first = first_ref[step]
    count = count_ref[step]
    places = lax.broadcasted_iota(jnp.int32, (rows, width), 1)
    distance = places - low_ref[...]
    span = span_ref[...]

    top[...] = jnp.full(top.shape, LEAST, jnp.float32)

    def score(tile, carry):
        start = pl.multiple_of(first + tile * width, GRAIN)
        away = distance + start
        allowed = (away >= 0) & (away < span)
        for head in range(heads):
            lower = head * HEAD_DIM
            part = lax.dot_general(
                q_ref[:, lower:lower + HEAD_DIM], keys[pl.ds(start, width), lower:lower + HEAD_DIM],
                (((1,), (1,)), ((), ())), preferred_element_type=jnp.float32)
            part = jnp.where(allowed, part, LEAST)
            scores[tile, head] = part
            best = top[head]
            for chunk in range(width // HEAD_DIM):
                best = jnp.maximum(best, part[:, chunk * HEAD_DIM:(chunk + 1) * HEAD_DIM])
            top[head] = best
        return carry

    lax.fori_loop(0, count, score, 0)
    for head in range(heads):
        top[head] = jnp.broadcast_to(jnp.max(top[head], axis=1, keepdims=True), top.shape[1:])
    gathered[...] = jnp.zeros_like(gathered)

    def mix(tile, carry):
        start = pl.multiple_of(first + tile * width, GRAIN)
        for head in range(heads):
            lower = 2 * head * HEAD_DIM
            best = jnp.concatenate([top[head]] * (width // HEAD_DIM), axis=1)
            weights = jnp.exp2((scores[tile, head] - best) * factor)
            gathered[head] += jnp.dot(
                weights.astype(jnp.bfloat16), mixed[pl.ds(start, width), lower:lower + 2 * HEAD_DIM],
                preferred_element_type=jnp.float32)
        return carry

    lax.fori_loop(0, count, mix, 0)
    for head in range(heads):
        lower = head * HEAD_DIM
        result = gathered[head]
        out_ref[:, lower:lower + HEAD_DIM] = (
            result[:, :HEAD_DIM] / result[:, HEAD_DIM:]).astype(out_ref.dtype)


def attend(first, count, low, span, queries, key_parts, value_parts, tile_rows, width):
    rows, columns = queries.shape
    heads = columns // HEAD_DIM
    held = sum(part.shape[0] for part in key_parts)
    window = held + width
    most = -(-(GRAIN + DOC_MOST + tile_rows + IMG_LEN) // width)
    whole = [pl.BlockSpec(part.shape, lambda i, *_: (0, 0)) for part in (*key_parts, *value_parts)]
    tiles = [pl.BlockSpec((tile_rows, size), lambda i, *_: (i, 0)) for size in (1, 1, columns)]
    return pl.pallas_call(
        functools.partial(attend_kernel, heads=heads, width=width),
        out_shape=jax.ShapeDtypeStruct((rows, columns), queries.dtype),
        grid_spec=pltpu.PrefetchScalarGridSpec(
            num_scalar_prefetch=2, grid=(rows // tile_rows,),
            in_specs=tiles + whole,
            out_specs=pl.BlockSpec((tile_rows, columns), lambda i, *_: (i, 0)),
            scratch_shapes=[
                pltpu.VMEM((window, columns), queries.dtype),
                pltpu.VMEM((window, 2 * columns), queries.dtype),
                pltpu.VMEM((most, heads, tile_rows, width), jnp.float32),
                pltpu.VMEM((heads, tile_rows, HEAD_DIM), jnp.float32),
                pltpu.VMEM((heads, tile_rows, 2 * HEAD_DIM), jnp.float32),
            ]),
        compiler_params=pltpu.CompilerParams(
            dimension_semantics=("arbitrary",), vmem_limit_bytes=56 * 2**20),
        cost_estimate=pl.CostEstimate(
            flops=4 * rows * 640 * columns, bytes_accessed=2 * (2 * rows + 2 * held) * columns,
            transcendentals=rows * 640 * heads),
        name="attend",
    )(first, count, low, span, queries, *key_parts, *value_parts)


def whole_step(queries, key_rows, values, doc_ids, image_flags, labels, token_loss):
    group = ("pair", "head")
    members = lax.axis_size("pair") * lax.axis_size("head")
    local_rows = queries.shape[0]
    rows = local_rows * members
    tile_rows, width = 256, 256

    exchange = functools.partial(lax.all_to_all, axis_name=group, split_axis=1, concat_axis=0, tiled=True)
    back = round_up(DOC_MOST - 1, GRAIN)
    ahead = round_up(IMG_LEN - 1, GRAIN)
    keys = exchange(key_rows)
    vals = exchange(values)
    quer = exchange(queries)
    key_back = shifted(keys[rows - back:], "outer", 1)
    key_ahead = shifted(keys[:ahead], "outer", -1)
    value_back = shifted(vals[rows - back:], "outer", 1)
    value_ahead = shifted(vals[:ahead], "outer", -1)
    key_parts = (key_back, keys, key_ahead)
    value_parts = (value_back, vals, value_ahead)

    documents = doc_ids.shape[0] // DOC_MEAN
    numbers = jnp.arange(documents, dtype=jnp.int32)[:, None]
    places = jnp.arange(doc_ids.shape[0], dtype=jnp.int32)[None, :]
    starts = jnp.sum((doc_ids[None, :] < numbers).astype(jnp.int32), axis=1, keepdims=True)
    image = (doc_ids[None, :] == numbers) & (image_flags[None, :] == 1)
    image_ends = jnp.max(jnp.where(image, places + 1, 0), axis=1, keepdims=True)
    block_start = lax.axis_index("outer") * rows
    block_docs = lax.dynamic_slice_in_dim(doc_ids, block_start, rows)[None, :]
    block_flags = lax.dynamic_slice_in_dim(image_flags, block_start, rows)
    own = block_docs == numbers
    low = jnp.sum(jnp.where(own, starts, 0), axis=0)
    image_high = jnp.sum(jnp.where(own, image_ends, 0), axis=0)
    high = jnp.where(block_flags == 1, image_high, block_start + jnp.arange(rows, dtype=jnp.int32) + 1)
    low = low - (block_start - back)
    high = high - (block_start - back)
    first = low[::tile_rows] // GRAIN * GRAIN
    last = jnp.max(high.reshape(-1, tile_rows), axis=1)
    count = (last - first + width - 1) // width

    attended = attend(first, count, low[:, None], (high - low)[:, None], quer, key_parts, value_parts, tile_rows, width)
    output = lax.all_to_all(attended, group, split_axis=0, concat_axis=1, tiled=True)

    row_start = block_start + (lax.axis_index("pair") * lax.axis_size("head") + lax.axis_index("head")) * local_rows
    local_docs = lax.dynamic_slice_in_dim(doc_ids, row_start, local_rows)
    member = (local_docs[:, None] == numbers.T) & (labels[:, None] >= 0)
    counts = jnp.sum(member.astype(jnp.float32), axis=0)
    sums = jnp.sum(jnp.where(member, token_loss[:, None], jnp.float32(0.0)), axis=0)
    totals = jnp.stack([counts, sums])
    for axis in ("head", "pair", "outer"):
        totals = summed(totals, axis)
    counts, sums = totals
    return (output, counts, sums / jnp.maximum(counts, jnp.float32(1.0)))


def solution(mesh):
    blocks, heads = mesh.shape["seq"], mesh.shape["head"]
    pair = 2 if blocks % 2 == 0 else 1
    fine = Mesh(mesh.devices.reshape(blocks // pair, pair, heads), ("outer", "pair", "head"))
    tokens = ("outer", "pair", "head")
    in_specs = (P(tokens, None), P(tokens, None), P(tokens, None), P(), P(), P(tokens), P(tokens))
    out_specs = (P(tokens, None), P(), P())
    return jax.shard_map(whole_step, mesh=fine, in_specs=in_specs, out_specs=out_specs, check_vma=False)
```

```python
import functools
import math

import jax
import jax.numpy as jnp
from jax import lax
from jax.experimental import pallas as pl
from jax.experimental.pallas import tpu as pltpu
from jax.sharding import Mesh, PartitionSpec as P

HEAD_DIM = 128
DOC_MEAN = 384
DOC_MOST = 704
IMG_LEN = 576
LEAST = -1e30
GRAIN = 16
HALO_GRAIN = 64
HALVES = 2
VMEM_LIMIT = 20 * 2**20


def round_up(count, grain):
    return -(-count // grain) * grain


def shifted(block, axis, distance):
    devices = range(lax.axis_size(axis))
    route = [(i - distance, i) for i in devices if i - distance in devices]
    return lax.ppermute(block, axis, route)


def summed(totals, axis):
    size = lax.axis_size(axis)
    if size & (size - 1):
        return lax.psum(totals, axis)
    distance = 1
    while distance < size:
        totals = totals + lax.ppermute(totals, axis, [(i, i ^ distance) for i in range(size)])
        distance *= 2
    return totals


def column(ref, step, rows):
    lines = rows // HEAD_DIM
    tall = [
        jnp.broadcast_to(ref[pl.ds(step * lines + line, 1), :], (HEAD_DIM, HEAD_DIM)).T
        for line in range(lines)
    ]
    return jnp.concatenate(tall, axis=0)


def attend_kernel(
    plan_ref, low_ref, span_ref, queries_ref, back_ref, own_ref, ahead_ref,
    out_ref, plan, query, keys, vals, scores, top, gathered, ready, sent, came, *, heads, width, common, place,
):
    step = pl.program_id(0)
    rows = ready.shape[1]
    steps = out_ref.shape[0] // rows
    window = keys.shape[0]
    factor = HEAD_DIM ** (-0.5) * math.log2(math.e)

    back, own, ahead = back_ref.shape[0], own_ref.shape[0], ahead_ref.shape[0]
    held = back + own + ahead
    columns = keys.shape[1]

    def halo(side, target):
        lower = side * columns
        return [
            pltpu.make_async_copy(
                part.at[:, lower:lower + columns], target.at[start:start + part.shape[0], :],
                came.at[2 + 2 * side + index])
            for index, (part, start) in enumerate(((back_ref, 0), (ahead_ref, back + own)))
        ]

    needs = [
        pltpu.make_async_copy(plan_ref, plan, came.at[0]),
        pltpu.make_async_copy(
            queries_ref.at[:, place * columns:(place + 1) * columns], query, came.at[1]),
    ] + halo(0, keys)
    rest = halo(1, vals)

    @pl.when(step == 0)
    def _():
        for move in needs + rest:
            move.start()
        for side, target in enumerate((keys, vals)):
            lower = (2 * place + side) * columns
            target[back:back + own, :] = own_ref[:, lower:lower + columns]
            target[held:, :] = jnp.zeros((window - held, columns), target.dtype)
        for move in needs:
            move.wait()

    first = plan[0, step]
    count = plan[1, step]
    tile = pl.ds(pl.multiple_of(step * rows, rows), rows)
    lanes = lax.broadcasted_iota(jnp.int32, (rows, HEAD_DIM), 1)
    above = lanes - column(low_ref, step, rows)
    below = above - column(span_ref, step, rows)

    def score(turn, tiles, fresh):
        start = pl.multiple_of(first + turn * width, GRAIN)
        for head in range(heads):
            lower = head * HEAD_DIM
            part = lax.dot_general(
                query[tile, lower:lower + HEAD_DIM], keys[pl.ds(start, tiles * width), lower:lower + HEAD_DIM],
                (((1,), (1,)), ((), ())), preferred_element_type=jnp.float32)
            best = None if fresh else top[head]
            for chunk in range(tiles * width // HEAD_DIM):
                cut = -(start + chunk * HEAD_DIM)
                piece = part[:, chunk * HEAD_DIM:(chunk + 1) * HEAD_DIM]
                piece = jnp.where((above >= cut) & (below < cut), piece, LEAST)
                scores[turn * per_tile + chunk, head] = piece
                best = piece if best is None else jnp.maximum(best, piece)
            top[head] = best

    per_tile = width // HEAD_DIM
    score(0, common, True)

    @pl.loop(common, count)
    def _(tile):
        score(tile, 1, False)

    for head in range(heads):
        top[head] = jnp.broadcast_to(jnp.max(top[head], axis=1, keepdims=True), top.shape[1:])

    @pl.when(step == 0)
    def _():
        for move in rest:
            move.wait()

    def mix(turn, tiles, fresh):
        start = pl.multiple_of(first + turn * width, GRAIN)
        ones = jnp.ones((tiles * width, HEAD_DIM), vals.dtype)
        for head in range(heads):
            lower = head * HEAD_DIM
            best = top[head]
            weights = jnp.concatenate([
                jnp.exp2((scores[turn * per_tile + chunk, head] - best) * factor).astype(jnp.bfloat16)
                for chunk in range(tiles * per_tile)], axis=1)
            found = jnp.dot(
                weights, jnp.concatenate([vals[pl.ds(start, tiles * width), lower:lower + HEAD_DIM], ones], axis=1),
                preferred_element_type=jnp.float32)
            gathered[head] = found if fresh else gathered[head] + found

    mix(0, common, True)

    @pl.loop(common, count)
    def _(tile):
        mix(tile, 1, False)

    slot = lax.rem(step, 2)

    def leaving(index, place):
        return pltpu.make_async_copy(
            ready.at[place], out_ref.at[pl.ds(pl.multiple_of(index * rows, rows), rows), :], sent.at[place])

    @pl.when(step >= 2)
    def _():
        leaving(step - 2, slot).wait()

    for head in range(heads):
        lower = head * HEAD_DIM
        result = gathered[head]
        ready[slot, :, lower:lower + HEAD_DIM] = (
            result[:, :HEAD_DIM] / result[:, HEAD_DIM:]).astype(ready.dtype)
    leaving(step, slot).start()

    @pl.when(step == steps - 1)
    def _():
        if steps > 1:
            leaving(step - 1, 1 - slot).wait()
        leaving(step, slot).wait()


def distant(array):
    return pltpu.with_memory_space_constraint(array, pltpu.HBM)


def attend(plan, low, span, queries, parts, place, tile_rows, width):
    rows, columns = queries.shape[0], parts[0].shape[1] // 2
    heads = columns // HEAD_DIM
    held = sum(part.shape[0] for part in parts)
    common = -(-(GRAIN + DOC_MOST) // width)
    window = held + max(width, common * width - parts[-1].shape[0])
    most = -(-(GRAIN + DOC_MOST + tile_rows + IMG_LEN) // width)
    near = pl.BlockSpec(memory_space=pltpu.VMEM)
    far = pl.BlockSpec(memory_space=pltpu.HBM)
    return pl.pallas_call(
        functools.partial(attend_kernel, heads=heads, width=width, common=common, place=place),
        out_shape=pltpu.HBM((rows, columns), queries.dtype),
        grid=(rows // tile_rows,),
        in_specs=[far, near, near, far, far, near, far],
        out_specs=far,
        scratch_shapes=[
            pltpu.SMEM(plan.shape, plan.dtype),
            pltpu.VMEM((rows, columns), queries.dtype),
            pltpu.VMEM((window, columns), queries.dtype),
            pltpu.VMEM((window, columns), queries.dtype),
            pltpu.VMEM((most * width // HEAD_DIM, heads, tile_rows, HEAD_DIM), jnp.float32),
            pltpu.VMEM((heads, tile_rows, HEAD_DIM), jnp.float32),
            pltpu.VMEM((heads, tile_rows, 2 * HEAD_DIM), jnp.float32),
            pltpu.VMEM((2, tile_rows, columns), queries.dtype),
            pltpu.SemaphoreType.DMA((2,)),
            pltpu.SemaphoreType.DMA((6,)),
        ],
        compiler_params=pltpu.CompilerParams(
            dimension_semantics=("arbitrary",), vmem_limit_bytes=VMEM_LIMIT),
        cost_estimate=pl.CostEstimate(
            flops=4 * rows * 640 * columns, bytes_accessed=2 * (2 * rows + 2 * held) * columns,
            transcendentals=rows * 640 * heads),
    )(distant(plan), low, span, distant(queries), distant(parts[0]), parts[1], distant(parts[2]))


def spread_kernel(key_ref, value_ref, target_ref, held, came, went):
    parts, rows, columns = held.shape
    piece = columns // (2 * HALVES)

    def coming(part):
        return [
            pltpu.make_async_copy(
                source.at[:, (part * HALVES + half) * piece:(part * HALVES + half + 1) * piece],
                held.at[part, :, (2 * half + side) * piece:(2 * half + side + 1) * piece],
                came.at[part, 2 * half + side])
            for half in range(HALVES) for side, source in enumerate((key_ref, value_ref))
        ]

    def going(part):
        return pltpu.make_async_copy(
            held.at[part], target_ref.at[part * rows:(part + 1) * rows, :], went.at[part])

    for part in range(parts):
        for move in coming(part):
            move.start()
    for part in range(parts):
        for move in coming(part):
            move.wait()
        going(part).start()
    for part in range(parts):
        going(part).wait()


def spread(key_rows, values, parts):
    rows, columns = key_rows.shape
    share = 2 * columns // parts
    return pl.pallas_call(
        spread_kernel,
        out_shape=pltpu.HBM((rows * parts, share), key_rows.dtype),
        in_specs=[pl.BlockSpec(memory_space=pltpu.HBM)] * 2,
        out_specs=pl.BlockSpec(memory_space=pltpu.HBM),
        scratch_shapes=[
            pltpu.VMEM((parts, rows, share), key_rows.dtype),
            pltpu.SemaphoreType.DMA((parts, 2 * HALVES)),
            pltpu.SemaphoreType.DMA((parts,)),
        ],
        compiler_params=pltpu.CompilerParams(vmem_limit_bytes=8 * 2**20),
        cost_estimate=pl.CostEstimate(flops=2**20, bytes_accessed=8 * rows * columns, transcendentals=0),
        name="spread",
    )(distant(key_rows), distant(values))


def weave_kernel(part_ref, *refs, parts, half):
    out_ref, sems = refs[-2:]
    rows, piece = part_ref.shape[0] // parts, part_ref.shape[1]
    moves = [
        pltpu.make_async_copy(
            part_ref.at[part * rows:(part + 1) * rows, :],
            out_ref.at[:, (part * HALVES + half) * piece:(part * HALVES + half + 1) * piece], sems.at[part])
        for part in range(parts)
    ]
    for move in moves:
        move.start()
    for move in moves:
        move.wait()


def weave(array, half, parts, before):
    rows, piece = array.shape
    far = pl.BlockSpec(memory_space=pltpu.HBM)
    return pl.pallas_call(
        functools.partial(weave_kernel, parts=parts, half=half),
        out_shape=pltpu.HBM((rows // parts, piece * parts * HALVES), array.dtype),
        in_specs=[pl.BlockSpec(memory_space=pltpu.VMEM)] + [far] * len(before),
        out_specs=far,
        scratch_shapes=[pltpu.SemaphoreType.DMA((parts,))],
        input_output_aliases={1: 0} if before else {},
        compiler_params=pltpu.CompilerParams(vmem_limit_bytes=8 * 2**20),
        cost_estimate=pl.CostEstimate(flops=2**20, bytes_accessed=4 * rows * piece, transcendentals=0),
    )(array, *before)


def whole_step(queries, key_rows, values, doc_ids, image_flags, labels, token_loss):
    group = ("pair", "head")
    members = lax.axis_size("pair") * lax.axis_size("head")
    local_rows = queries.shape[0]
    rows = local_rows * members
    tile_rows, width = 256, 256

    back = round_up(DOC_MOST - 1, HALO_GRAIN)
    ahead = round_up(IMG_LEN - 1, HALO_GRAIN)
    pairs = lax.all_to_all(spread(key_rows, values, members), group, split_axis=0, concat_axis=0, tiled=True)
    quer = lax.all_to_all(queries, group, split_axis=1, concat_axis=0, tiled=True)
    columns = quer.shape[1]
    halos = []
    for half in range(HALVES):
        lower = half * 2 * columns // HALVES
        upper = lower + 2 * columns // HALVES
        behind = shifted(pairs[rows - back:, lower:upper], "outer", 1)
        front = shifted(pairs[:ahead, lower:upper], "outer", -1)
        halos.append((behind, front))

    documents = doc_ids.shape[0] // DOC_MEAN
    numbers = jnp.arange(documents, dtype=jnp.int32)[:, None]
    places = jnp.arange(doc_ids.shape[0], dtype=jnp.int32)[None, :]
    starts = jnp.sum((doc_ids[None, :] < numbers).astype(jnp.int32), axis=1, keepdims=True)
    image = (doc_ids[None, :] == numbers) & (image_flags[None, :] == 1)
    image_ends = jnp.max(jnp.where(image, places + 1, 0), axis=1, keepdims=True)
    block_start = lax.axis_index("outer") * rows
    block_docs = lax.dynamic_slice_in_dim(doc_ids, block_start, rows)[None, :]
    block_flags = lax.dynamic_slice_in_dim(image_flags, block_start, rows)
    own = block_docs == numbers
    low = jnp.sum(jnp.where(own, starts, 0), axis=0)
    image_high = jnp.sum(jnp.where(own, image_ends, 0), axis=0)
    high = jnp.where(block_flags == 1, image_high, block_start + jnp.arange(rows, dtype=jnp.int32) + 1)
    low = low - (block_start - back)
    high = high - (block_start - back)
    first = low[::tile_rows] // GRAIN * GRAIN
    last = jnp.max(high.reshape(-1, tile_rows), axis=1)
    plan = jnp.stack([first, (last - first + width - 1) // width])

    low, span = low.reshape(-1, HEAD_DIM), (high - low).reshape(-1, HEAD_DIM)
    woven = ()
    for half, (behind, front) in enumerate(halos):
        attended = attend(plan, low, span, quer, (behind, pairs, front), half, tile_rows, width)
        result = lax.all_to_all(attended, group, split_axis=0, concat_axis=0, tiled=True)
        woven = (weave(result, half, members, woven),)
    output, = woven

    row_start = block_start + (lax.axis_index("pair") * lax.axis_size("head") + lax.axis_index("head")) * local_rows
    local_docs = lax.dynamic_slice_in_dim(doc_ids, row_start, local_rows)
    member = (local_docs[:, None] == numbers.T) & (labels[:, None] >= 0)
    counts = jnp.sum(member.astype(jnp.float32), axis=0)
    sums = jnp.sum(jnp.where(member, token_loss[:, None], jnp.float32(0.0)), axis=0)
    totals = jnp.stack([counts, sums])
    for axis in ("outer", "head", "pair"):
        totals = summed(totals, axis)
    counts, sums = totals
    return (output, counts, sums / jnp.maximum(counts, jnp.float32(1.0)))


def solution(mesh):
    blocks, heads = mesh.shape["seq"], mesh.shape["head"]
    pair = 2 if blocks % 2 == 0 else 1
    fine = Mesh(mesh.devices.reshape(blocks // pair, pair, heads), ("outer", "pair", "head"))
    tokens = ("outer", "pair", "head")
    in_specs = (P(tokens, None), P(tokens, None), P(tokens, None), P(), P(), P(tokens), P(tokens))
    out_specs = (P(tokens, None), P(), P())
    return jax.shard_map(whole_step, mesh=fine, in_specs=in_specs, out_specs=out_specs, check_vma=False)
```

```python
import functools
import math

import jax
import jax.numpy as jnp
from jax import lax
from jax.experimental import pallas as pl
from jax.experimental.pallas import tpu as pltpu
from jax.sharding import Mesh, PartitionSpec as P

HEAD_DIM = 128
DOC_MEAN = 384
DOC_MOST = 704
IMG_LEN = 576
LEAST = -1e30
GRAIN = 16
HALO_GRAIN = 64
HALVES = 2
VMEM_LIMIT = 20 * 2**20


def round_up(count, grain):
    return -(-count // grain) * grain


def shifted(block, axis, distance):
    devices = range(lax.axis_size(axis))
    route = [(i - distance, i) for i in devices if i - distance in devices]
    return lax.ppermute(block, axis, route)


def summed(totals, axis):
    size = lax.axis_size(axis)
    if size & (size - 1):
        return lax.psum(totals, axis)
    distance = 1
    while distance < size:
        totals = totals + lax.ppermute(totals, axis, [(i, i ^ distance) for i in range(size)])
        distance *= 2
    return totals


def column(ref, step, rows):
    lines = rows // HEAD_DIM
    tall = [
        jnp.broadcast_to(ref[pl.ds(step * lines + line, 1), :], (HEAD_DIM, HEAD_DIM)).T
        for line in range(lines)
    ]
    return jnp.concatenate(tall, axis=0)


def attend_kernel(
    plan_ref, low_ref, span_ref, queries_ref, back_ref, own_ref, ahead_ref,
    out_ref, plan, query, keys, vals, scores, top, gathered, ready, sent, came, *, heads, width, common, place,
):
    step = pl.program_id(0)
    rows = ready.shape[1]
    steps = out_ref.shape[0] // rows
    window = keys.shape[0]
    factor = HEAD_DIM ** (-0.5) * math.log2(math.e)

    back, own, ahead = back_ref.shape[0], own_ref.shape[0], ahead_ref.shape[0]
    held = back + own + ahead
    columns = keys.shape[1]

    def halo(side, target):
        lower = side * columns
        return [
            pltpu.make_async_copy(
                part.at[:, lower:lower + columns], target.at[start:start + part.shape[0], :],
                came.at[2 + 2 * side + index])
            for index, (part, start) in enumerate(((back_ref, 0), (ahead_ref, back + own)))
        ]

    needs = [
        pltpu.make_async_copy(plan_ref, plan, came.at[0]),
        pltpu.make_async_copy(
            queries_ref.at[:, place * columns:(place + 1) * columns], query, came.at[1]),
    ] + halo(0, keys)
    rest = halo(1, vals)

    @pl.when(step == 0)
    def _():
        for move in needs + rest:
            move.start()
        for side, target in enumerate((keys, vals)):
            lower = (2 * place + side) * columns
            target[back:back + own, :] = own_ref[:, lower:lower + columns]
            target[held:, :] = jnp.zeros((window - held, columns), target.dtype)
        for move in needs + rest:
            move.wait()

    lanes = lax.broadcasted_iota(jnp.int32, (rows, HEAD_DIM), 1)
    above = lanes - column(low_ref, step, rows)
    below = above - column(span_ref, step, rows)

    per_tile = width // HEAD_DIM

    def score(first, begin, size, turn, tiles, fresh):
        start = pl.multiple_of(first + turn * width, GRAIN)
        tile = pl.ds(pl.multiple_of(step * rows + begin, size), size)
        over, under = above[begin:begin + size], below[begin:begin + size]
        for head in range(heads):
            lower = head * HEAD_DIM
            part = lax.dot_general(
                query[tile, lower:lower + HEAD_DIM], keys[pl.ds(start, tiles * width), lower:lower + HEAD_DIM],
                (((1,), (1,)), ((), ())), preferred_element_type=jnp.float32)
            best = None if fresh else top[head, begin:begin + size]
            for chunk in range(tiles * per_tile):
                cut = -(start + chunk * HEAD_DIM)
                piece = part[:, chunk * HEAD_DIM:(chunk + 1) * HEAD_DIM]
                piece = jnp.where((over >= cut) & (under < cut), piece, LEAST)
                scores[turn * per_tile + chunk, head, begin:begin + size] = piece
                best = piece if best is None else jnp.maximum(best, piece)
            top[head, begin:begin + size] = best

    def settle(begin, size):
        for head in range(heads):
            best = top[head, begin:begin + size]
            top[head, begin:begin + size] = jnp.broadcast_to(jnp.max(best, axis=1, keepdims=True), best.shape)

    def mix(first, begin, size, turn, tiles, fresh):
        start = pl.multiple_of(first + turn * width, GRAIN)
        ones = jnp.ones((tiles * width, HEAD_DIM), vals.dtype)
        for head in range(heads):
            lower = head * HEAD_DIM
            best = top[head, begin:begin + size]
            weights = jnp.concatenate([
                jnp.exp2((scores[turn * per_tile + chunk, head, begin:begin + size] - best) * factor)
                .astype(jnp.bfloat16)
                for chunk in range(tiles * per_tile)], axis=1)
            found = jnp.dot(
                weights, jnp.concatenate([vals[pl.ds(start, tiles * width), lower:lower + HEAD_DIM], ones], axis=1),
                preferred_element_type=jnp.float32)
            gathered[head, begin:begin + size] = found if fresh else gathered[head, begin:begin + size] + found

    half = rows // 2
    origin = plan[0, 2 * step]
    extent = jnp.maximum(plan[1, 2 * step], plan[1, 2 * step + 1]) - origin

    @pl.when(extent <= common * width)
    def _():
        score(origin, 0, rows, 0, common, True)
        settle(0, rows)
        mix(origin, 0, rows, 0, common, True)

    @pl.when(extent > common * width)
    def _():
        for side in range(2):
            begin = side * half
            first = plan[0, 2 * step + side]
            count = (plan[1, 2 * step + side] - first + width - 1) // width
            score(first, begin, half, 0, common, True)

            @pl.loop(common, count)
            def _(turn):
                score(first, begin, half, turn, 1, False)

            settle(begin, half)
            mix(first, begin, half, 0, common, True)

            @pl.loop(common, count)
            def _(turn):
                mix(first, begin, half, turn, 1, False)

    slot = lax.rem(step, 2)

    def leaving(index, place):
        return pltpu.make_async_copy(
            ready.at[place], out_ref.at[pl.ds(pl.multiple_of(index * rows, rows), rows), :], sent.at[place])

    @pl.when(step >= 2)
    def _():
        leaving(step - 2, slot).wait()

    for head in range(heads):
        lower = head * HEAD_DIM
        result = gathered[head]
        ready[slot, :, lower:lower + HEAD_DIM] = (
            result[:, :HEAD_DIM] / result[:, HEAD_DIM:]).astype(ready.dtype)
    leaving(step, slot).start()

    @pl.when(step == steps - 1)
    def _():
        if steps > 1:
            leaving(step - 1, 1 - slot).wait()
        leaving(step, slot).wait()


def distant(array):
    return pltpu.with_memory_space_constraint(array, pltpu.HBM)


def attend(plan, low, span, queries, parts, place, tile_rows, width):
    rows, columns = queries.shape[0], parts[0].shape[1] // 2
    heads = columns // HEAD_DIM
    held = sum(part.shape[0] for part in parts)
    common = -(-(GRAIN + DOC_MOST) // width)
    window = held + max(width, common * width - parts[-1].shape[0])
    most = -(-(GRAIN + DOC_MOST + tile_rows + IMG_LEN) // width)
    near = pl.BlockSpec(memory_space=pltpu.VMEM)
    far = pl.BlockSpec(memory_space=pltpu.HBM)
    return pl.pallas_call(
        functools.partial(attend_kernel, heads=heads, width=width, common=common, place=place),
        out_shape=pltpu.HBM((rows, columns), queries.dtype),
        grid=(rows // tile_rows,),
        in_specs=[far, near, near, far, far, near, far],
        out_specs=far,
        scratch_shapes=[
            pltpu.SMEM(plan.shape, plan.dtype),
            pltpu.VMEM((rows, columns), queries.dtype),
            pltpu.VMEM((window, columns), queries.dtype),
            pltpu.VMEM((window, columns), queries.dtype),
            pltpu.VMEM((most * width // HEAD_DIM, heads, tile_rows, HEAD_DIM), jnp.float32),
            pltpu.VMEM((heads, tile_rows, HEAD_DIM), jnp.float32),
            pltpu.VMEM((heads, tile_rows, 2 * HEAD_DIM), jnp.float32),
            pltpu.VMEM((2, tile_rows, columns), queries.dtype),
            pltpu.SemaphoreType.DMA((2,)),
            pltpu.SemaphoreType.DMA((6,)),
        ],
        compiler_params=pltpu.CompilerParams(
            dimension_semantics=("arbitrary",), vmem_limit_bytes=VMEM_LIMIT),
        cost_estimate=pl.CostEstimate(
            flops=4 * rows * 640 * columns, bytes_accessed=2 * (2 * rows + 2 * held) * columns,
            transcendentals=rows * 640 * heads),
    )(distant(plan), low, span, distant(queries), distant(parts[0]), parts[1], distant(parts[2]))


def spread_kernel(key_ref, value_ref, target_ref, held, came, went):
    parts, rows, columns = held.shape
    piece = columns // (2 * HALVES)

    def coming(part):
        return [
            pltpu.make_async_copy(
                source.at[:, (part * HALVES + half) * piece:(part * HALVES + half + 1) * piece],
                held.at[part, :, (2 * half + side) * piece:(2 * half + side + 1) * piece],
                came.at[part, 2 * half + side])
            for half in range(HALVES) for side, source in enumerate((key_ref, value_ref))
        ]

    def going(part):
        return pltpu.make_async_copy(
            held.at[part], target_ref.at[part * rows:(part + 1) * rows, :], went.at[part])

    for part in range(parts):
        for move in coming(part):
            move.start()
    for part in range(parts):
        for move in coming(part):
            move.wait()
        going(part).start()
    for part in range(parts):
        going(part).wait()


def spread(key_rows, values, parts):
    rows, columns = key_rows.shape
    share = 2 * columns // parts
    return pl.pallas_call(
        spread_kernel,
        out_shape=pltpu.HBM((rows * parts, share), key_rows.dtype),
        in_specs=[pl.BlockSpec(memory_space=pltpu.HBM)] * 2,
        out_specs=pl.BlockSpec(memory_space=pltpu.HBM),
        scratch_shapes=[
            pltpu.VMEM((parts, rows, share), key_rows.dtype),
            pltpu.SemaphoreType.DMA((parts, 2 * HALVES)),
            pltpu.SemaphoreType.DMA((parts,)),
        ],
        compiler_params=pltpu.CompilerParams(vmem_limit_bytes=8 * 2**20),
        cost_estimate=pl.CostEstimate(flops=2**20, bytes_accessed=8 * rows * columns, transcendentals=0),
        name="spread",
    )(distant(key_rows), distant(values))


def weave_kernel(part_ref, *refs, parts, half):
    out_ref, sems = refs[-2:]
    rows, piece = part_ref.shape[0] // parts, part_ref.shape[1]
    moves = [
        pltpu.make_async_copy(
            part_ref.at[part * rows:(part + 1) * rows, :],
            out_ref.at[:, (part * HALVES + half) * piece:(part * HALVES + half + 1) * piece], sems.at[part])
        for part in range(parts)
    ]
    for move in moves:
        move.start()
    for move in moves:
        move.wait()


def weave(array, half, parts, before):
    rows, piece = array.shape
    far = pl.BlockSpec(memory_space=pltpu.HBM)
    return pl.pallas_call(
        functools.partial(weave_kernel, parts=parts, half=half),
        out_shape=pltpu.HBM((rows // parts, piece * parts * HALVES), array.dtype),
        in_specs=[pl.BlockSpec(memory_space=pltpu.VMEM)] + [far] * len(before),
        out_specs=far,
        scratch_shapes=[pltpu.SemaphoreType.DMA((parts,))],
        input_output_aliases={1: 0} if before else {},
        compiler_params=pltpu.CompilerParams(vmem_limit_bytes=8 * 2**20),
        cost_estimate=pl.CostEstimate(flops=2**20, bytes_accessed=4 * rows * piece, transcendentals=0),
    )(array, *before)


def cut_kernel(source_ref, tail_ref, head_ref, sems, *, lower):
    rows, columns = source_ref.shape[0], tail_ref.shape[1]
    moves = [
        pltpu.make_async_copy(
            source_ref.at[start:start + target.shape[0], lower:lower + columns], target, sems.at[index])
        for index, (start, target) in enumerate(((rows - tail_ref.shape[0], tail_ref), (0, head_ref)))
    ]
    for move in moves:
        move.start()
    for move in moves:
        move.wait()


def cut(array, back, ahead, half):
    columns = array.shape[1] // HALVES
    far = pl.BlockSpec(memory_space=pltpu.HBM)
    return pl.pallas_call(
        functools.partial(cut_kernel, lower=half * columns),
        out_shape=[pltpu.HBM((length, columns), array.dtype) for length in (back, ahead)],
        in_specs=[pl.BlockSpec(memory_space=pltpu.VMEM)],
        out_specs=[far, far],
        scratch_shapes=[pltpu.SemaphoreType.DMA((2,))],
        compiler_params=pltpu.CompilerParams(vmem_limit_bytes=6 * 2**20),
        cost_estimate=pl.CostEstimate(flops=2**20, bytes_accessed=4 * (back + ahead) * columns, transcendentals=0),
    )(array)


def whole_step(queries, key_rows, values, doc_ids, image_flags, labels, token_loss):
    group = ("pair", "head")
    members = lax.axis_size("pair") * lax.axis_size("head")
    local_rows = queries.shape[0]
    rows = local_rows * members
    tile_rows, width = 256, 256

    back = round_up(DOC_MOST - 1, HALO_GRAIN)
    ahead = round_up(IMG_LEN - 1, HALO_GRAIN)
    pairs = lax.all_to_all(spread(key_rows, values, members), group, split_axis=0, concat_axis=0, tiled=True)
    quer = lax.all_to_all(queries, group, split_axis=1, concat_axis=0, tiled=True)
    halos = []
    for half in range(HALVES):
        tail, head = cut(pairs, back, ahead, half)
        behind = shifted(tail, "outer", 1)
        front = shifted(head, "outer", -1)
        halos.append((behind, front))

    documents = doc_ids.shape[0] // DOC_MEAN
    numbers = jnp.arange(documents, dtype=jnp.int32)[:, None]
    places = jnp.arange(doc_ids.shape[0], dtype=jnp.int32)[None, :]
    starts = jnp.sum((doc_ids[None, :] < numbers).astype(jnp.int32), axis=1, keepdims=True)
    image = (doc_ids[None, :] == numbers) & (image_flags[None, :] == 1)
    image_ends = jnp.max(jnp.where(image, places + 1, 0), axis=1, keepdims=True)
    block_start = lax.axis_index("outer") * rows
    block_docs = lax.dynamic_slice_in_dim(doc_ids, block_start, rows)[None, :]
    block_flags = lax.dynamic_slice_in_dim(image_flags, block_start, rows)
    own = block_docs == numbers
    low = jnp.sum(jnp.where(own, starts, 0), axis=0)
    image_high = jnp.sum(jnp.where(own, image_ends, 0), axis=0)
    high = jnp.where(block_flags == 1, image_high, block_start + jnp.arange(rows, dtype=jnp.int32) + 1)
    low = low - (block_start - back)
    high = high - (block_start - back)
    half_rows = tile_rows // 2
    plan = jnp.stack([low[::half_rows] // GRAIN * GRAIN, jnp.max(high.reshape(-1, half_rows), axis=1)])

    low, span = low.reshape(-1, HEAD_DIM), (high - low).reshape(-1, HEAD_DIM)
    woven = ()
    for half, (behind, front) in enumerate(halos):
        attended = attend(plan, low, span, quer, (behind, pairs, front), half, tile_rows, width)
        result = lax.all_to_all(attended, group, split_axis=0, concat_axis=0, tiled=True)
        woven = (weave(result, half, members, woven),)
    output, = woven

    row_start = block_start + (lax.axis_index("pair") * lax.axis_size("head") + lax.axis_index("head")) * local_rows
    local_docs = lax.dynamic_slice_in_dim(doc_ids, row_start, local_rows)
    member = (local_docs[:, None] == numbers.T) & (labels[:, None] >= 0)
    counts = jnp.sum(member.astype(jnp.float32), axis=0)
    sums = jnp.sum(jnp.where(member, token_loss[:, None], jnp.float32(0.0)), axis=0)
    totals = jnp.stack([counts, sums])
    for axis in ("outer", "head", "pair"):
        totals = summed(totals, axis)
    counts, sums = totals
    return (output, counts, sums / jnp.maximum(counts, jnp.float32(1.0)))


def solution(mesh):
    blocks, heads = mesh.shape["seq"], mesh.shape["head"]
    pair = 2 if blocks % 2 == 0 else 1
    fine = Mesh(mesh.devices.reshape(blocks // pair, pair, heads), ("outer", "pair", "head"))
    tokens = ("outer", "pair", "head")
    in_specs = (P(tokens, None), P(tokens, None), P(tokens, None), P(), P(), P(tokens), P(tokens))
    out_specs = (P(tokens, None), P(), P())
    return jax.shard_map(whole_step, mesh=fine, in_specs=in_specs, out_specs=out_specs, check_vma=False)
```
